32 devices in a mesh: seq: 8 (over z, y), tp: 4 (over x, core).
Axes of the slice: x: 2, y: 2, z: 4, core: 2. Of those that a mesh axis runs over, the one named last changes fastest.
Arguments:
- latents: bfloat16 [1024, 3072], P('seq', 'tp'), may hold values from -6 to 6
- lengths: int32 [2], replicated, may hold values from 1 to 768, 1024 in all
- t_index: int32 [2], replicated, may hold values from 0 to 6
- mod_scale: float32 [3072], replicated, may hold values from -2 to 2
- q_weight: bfloat16 [3072, 2048], P(None, 'tp'), may hold values from -0.109375 to 0.109375
- k_weight: bfloat16 [3072, 2048], P(None, 'tp'), may hold values from -0.109375 to 0.109375
- v_weight: bfloat16 [3072, 2048], P(None, 'tp'), may hold values from -0.109375 to 0.109375
- out_weight: bfloat16 [2048, 3072], P('tp'), may hold values from -0.1875 to 0.1875
- q_gain: float32 [128], replicated, may hold values from 0.6 to 2.4
- k_gain: float32 [128], replicated, may hold values from 0.6 to 2.4
- student_weight: bfloat16 [3072, 3072], P('tp'), may hold values from -0.15625 to 0.15625
Outputs:
- target: bfloat16 [1024, 3072], P('seq', 'tp')
- student_velocity: bfloat16 [1024, 3072], P('seq', 'tp')
- loss: float32 [], replicated
The draws below stay inside these ranges and needn't reach their ends.
Inputs may be any that keep to these rules, and one draw needn't show every extreme that they name: lengths sum to 1024.
All inputs are finite; a program needn't handle non-finite values.
Results may differ from the reference program's by a relative error of at most 0.024.
Values may be sent and summed in bfloat16 or wider, within the bound.
No kernel may reach another device: no remote copies, remote signals or barrier semaphores. Data moves between devices by JAX's collectives and lax.ppermute only.
A program may use at most 64 MiB of HBM per device.

```python
import math
import jax
import jax.numpy as jnp
import numpy as np
from jax import lax

D = 3072
HEAD_DIM = 128
TGRID = 8
IMAGES = 2
INNER = 2048
TOKENS = 1024
MOST = 768
N_TP = 4


def gain_values(key):
    return jax.random.uniform(key, (HEAD_DIM,), jnp.float32, 0.6, 1.8)


def draw_q_gain(key, part):
    return gain_values(jax.random.fold_in(key, 11))


def draw_k_gain(key, part):
    return gain_values(jax.random.fold_in(key, 23))


def strengthened(values, key, source, target, shards_of, factor):
    owner, partner = [(jnp.arange(values.shape[position]) // (values.shape[position] // shards_of)).reshape([-1 if axis == position else 1 for axis in range(values.ndim)]) for position in (source, target)]
    chosen = jax.random.permutation(key, shards_of)[partner]
    strong = (owner == chosen) | (owner == (partner + shards_of // 2) % shards_of)
    return jnp.where(strong, factor * values, values)


def shard_levels(rng, dims, pieces, least, top_value):
    factor_of, own = 1.0, jax.random.fold_in(rng, 6)
    for position, shards_of in pieces:
        steps = jnp.exp(jax.random.uniform(jax.random.fold_in(own, position), (shards_of,), jnp.float32, least / len(pieces), top_value / len(pieces)))
        factor_of = factor_of * jnp.repeat(steps, dims[position] // shards_of).reshape([-1 if axis == position else 1 for axis in range(len(dims))])
    return factor_of


def split_up(amount, total, limit, slope):
    weights = [(1 << 20) // math.isqrt(standing ** slope) + 1 for standing in range(2, amount + 1)]
    rest, counts = total - limit - (amount - 1), [1] * (amount - 1)
    while rest > 0:
        free = [i for i in range(amount - 1) if counts[i] < limit]
        whole, remaining = sum([weights[i] for i in free]), rest
        for i in free:
            addition = min(limit - counts[i], max(1, remaining * weights[i] // whole), rest)
            counts[i] = counts[i] + addition
            rest = rest - addition
    return np.array([limit] + counts)


def uneven_parts(stream_key, count, total, limit, lean):
    if count == 2:
        one = jax.random.randint(stream_key, (), max(1, total - limit), min(limit, total - 1) + 1)
        return jnp.stack([one, total - one])
    tallies = jnp.asarray(split_up(count, total, limit, lean), jnp.int32)
    twos = (count - 1) // 2
    giver, sink = tallies[1:1 + 2 * twos:2], tallies[2:2 + 2 * twos:2]
    slack = jnp.minimum(giver - 1, limit - sink)
    passed = jax.random.randint(jax.random.fold_in(stream_key, 1), (twos,), 0, 1 << 20) % (slack + 1)
    tallies = tallies.at[1:1 + 2 * twos:2].set(giver - passed).at[2:2 + 2 * twos:2].set(sink + passed)
    return tallies[jax.random.permutation(jax.random.fold_in(stream_key, 2), count)]


def bell_draw(own_key, shape, spread, reach, split=(), kind=jnp.bfloat16):
    drawn = jax.random.normal(own_key, shape, jnp.float32) * spread
    if len(split) > 0:
        drawn = shard_levels(own_key, shape, split, -0.22, 0.18) * drawn
    return jnp.clip(drawn, min=-reach, max=reach).astype(kind)


def noise_with(own_key, dims, deviation, reach, split, heavy, held_as=jnp.bfloat16):
    array = deviation * jax.random.normal(own_key, dims, jnp.float32)
    if split:
        array = array * shard_levels(own_key, dims, split, -0.22, 0.18)
    return jnp.clip(strengthened(array, jax.random.fold_in(own_key, 3), *heavy), -reach, reach).astype(held_as)


def setup_inputs(seed: int = 0) -> dict:
    key_list = jax.random.split(jax.random.key(seed), 12)
    return {
        "latents": bell_draw(key_list[0], (TOKENS, D), 1.0, 6.0, ((0, 8), (1, 4))),
        "lengths": uneven_parts(key_list[1], IMAGES, TOKENS, MOST, 2).astype(jnp.int32),
        "t_index": jax.random.randint(key_list[2], (IMAGES,), 0, TGRID - 1).astype(jnp.int32),
        "mod_scale": jnp.clip(jax.random.uniform(key_list[3], (D,), jnp.float32, -2.0, 2.0), -2.0, 2.0),
        "q_weight": bell_draw(key_list[4], (D, INNER), D ** -0.5, 0.109375, ((1, 4),)),
        "k_weight": bell_draw(key_list[5], (D, INNER), D ** -0.5, 0.109375, ((1, 4),)),
        "v_weight": bell_draw(key_list[6], (D, INNER), D ** -0.5, 0.109375, ((1, 4),)),
        "out_weight": noise_with(key_list[7], (INNER, D), INNER ** -0.5, 0.1875, ((0, 4),), (0, 1, 4, 2.0)),
        "q_gain": draw_q_gain(jax.random.fold_in(key_list[11], 71), 0),
        "k_gain": draw_k_gain(jax.random.fold_in(key_list[11], 71), 0),
        "student_weight": noise_with(key_list[10], (D, D), D ** -0.5, 0.15625, ((0, 4),), (0, 1, 4, 2.0)),
    }


epsilon = 1e-06
kinetic_weight = 0.1

def image_index(positions, image_ends):
    return lax.optimization_barrier(jnp.sum((positions[:, None] >= image_ends[None, :]).astype(jnp.int32), axis=1)).astype(jnp.int32)

def head_norm(projected, gain):
    shaped = projected.reshape(projected.shape[0], -1, gain.shape[0])
    normed = shaped * lax.rsqrt(lax.optimization_barrier(jnp.mean(shaped * shaped, axis=-1, keepdims=True)) + epsilon) * gain
    return normed.astype(jnp.bfloat16)

def grouped_sum(left, right, groups):
    inner_width = left.shape[1] // groups

    def add_group(group, total):
        offset = (group * inner_width).astype(jnp.int32)
        columns = lax.dynamic_slice_in_dim(left, offset, inner_width, 1)
        block_rows = lax.dynamic_slice_in_dim(right, offset, inner_width, 0)
        term = jnp.dot(columns, block_rows, preferred_element_type=jnp.float32).astype(jnp.bfloat16)
        term = lax.optimization_barrier(term)
        return total + term.astype(jnp.float32)
    start_total = jnp.zeros((left.shape[0], right.shape[1]), jnp.float32)
    return lax.fori_loop(0, groups, add_group, start_total)

def attention(queries, key_rows, value_rows, image_of):
    score_scale = 1.0 / math.sqrt(queries.shape[2])
    same_image = image_of[:, None] == image_of[None, :]

    def one_head(triple):
        query_head, key_head, value_head = triple
        scores = jnp.dot(query_head, key_head.T, preferred_element_type=jnp.float32) * score_scale
        scores = jnp.where(same_image, scores, -1e+30)
        highest = lax.optimization_barrier(jnp.max(scores, axis=1, keepdims=True))
        weights = jnp.where(same_image, jnp.exp(scores - highest), 0.0)
        totals = lax.optimization_barrier(jnp.sum(weights, axis=1))
        mixed = jnp.dot(weights.astype(jnp.bfloat16), value_head, preferred_element_type=jnp.float32)
        return (mixed / totals[:, None]).astype(jnp.bfloat16)
    heads_out = lax.map(one_head, (queries.transpose(1, 0, 2), key_rows.transpose(1, 0, 2), value_rows.transpose(1, 0, 2)))
    return heads_out.transpose(1, 0, 2).reshape(queries.shape[0], -1)

def teacher(state, times, image_of, mod_scale, q_weight, k_weight, v_weight, out_weight, q_gain, k_gain):
    state32 = state.astype(jnp.float32)
    normed = state32 * lax.rsqrt(lax.optimization_barrier(jnp.mean(state32 * state32, axis=1, keepdims=True)) + epsilon)
    hidden = (normed * (1.0 + times[:, None] * mod_scale[None, :])).astype(jnp.bfloat16)
    queries = head_norm(jnp.dot(hidden, q_weight, preferred_element_type=jnp.float32), q_gain)
    key_rows = head_norm(jnp.dot(hidden, k_weight, preferred_element_type=jnp.float32), k_gain)
    value_rows = jnp.dot(hidden, v_weight, preferred_element_type=jnp.float32).astype(jnp.bfloat16)
    value_rows = value_rows.reshape(queries.shape)
    mixed = attention(queries, key_rows, value_rows, image_of)
    velocity = grouped_sum(mixed, out_weight, N_TP).astype(jnp.bfloat16)
    return (velocity, hidden)

def reference(latents, lengths, t_index, mod_scale, q_weight, k_weight, v_weight, out_weight, q_gain, k_gain, student_weight):
    positions = jnp.arange(TOKENS, dtype=jnp.int32)
    image_ends = jnp.cumsum(lengths).astype(jnp.int32)
    image_of = image_index(positions, image_ends)
    one_hot = (image_of[:, None] == jnp.arange(IMAGES, dtype=jnp.int32)[None, :]).astype(jnp.float32)
    start_times = lax.optimization_barrier(jnp.sum(one_hot * (t_index.astype(jnp.float32) / TGRID)[None, :], axis=1))
    step_size = 1.0 / TGRID
    first_velocity, first_hidden = teacher(latents, start_times, image_of, mod_scale, q_weight, k_weight, v_weight, out_weight, q_gain, k_gain)
    middle = (latents.astype(jnp.float32) + step_size * first_velocity.astype(jnp.float32)).astype(jnp.bfloat16)
    second_velocity, unused_hidden = teacher(middle, start_times + step_size, image_of, mod_scale, q_weight, k_weight, v_weight, out_weight, q_gain, k_gain)
    target = (0.5 * (first_velocity.astype(jnp.float32) + second_velocity.astype(jnp.float32))).astype(jnp.bfloat16)
    student_velocity = grouped_sum(first_hidden, student_weight, N_TP).astype(jnp.bfloat16)
    student32 = student_velocity.astype(jnp.float32)
    residual = student32 - target.astype(jnp.float32)
    per_token = lax.optimization_barrier(jnp.sum(residual * residual, axis=1)) + kinetic_weight * lax.optimization_barrier(jnp.sum(student32 * student32, axis=1))
    image_sum = lax.optimization_barrier(jnp.sum(one_hot * per_token[:, None], axis=0))
    loss = jnp.mean(image_sum / (lengths.astype(jnp.float32) * D))
    return (target, student_velocity, loss)
```

```python
import math

import jax
import jax.numpy as jnp
from jax import lax
from jax.sharding import PartitionSpec as P

TGRID = 8
epsilon = 1e-06
kinetic_weight = 0.1
F32, BF16 = jnp.float32, jnp.bfloat16


def image_index(positions, image_ends):
    return jnp.sum((positions[:, None] >= image_ends[None, :]).astype(jnp.int32), axis=1)


def swap(value, axis, size, mask):
    return lax.ppermute(value, axis, [(i, i ^ mask) for i in range(size)])


def bits_of(size):
    return [1 << b for b in range(size.bit_length() - 1)]


def gather_blocks(own, axis, size):
    blocks = {0: own}
    for bit in reversed(bits_of(size)):
        for k in list(blocks):
            blocks[k ^ bit] = swap(blocks[k], axis, size, bit)
    return [blocks[k] for k in range(size)]


def in_order(blocks, index):
    size = len(blocks)
    current = list(blocks)
    for bit in bits_of(size):
        flip = (index & bit) != 0
        current = [jnp.where(flip, current[k ^ bit], current[k]) for k in range(size)]
    return current


def reduce_blocks(terms, axis, size, keep_last):
    held = dict(enumerate(terms))
    bits = bits_of(size)
    for bit in bits:
        last = keep_last and bit == bits[-1]
        sent = {k: swap(held[k].astype(BF16), axis, size, bit) for k in held if last or k & bit}
        if last:
            held = {k: held[k].astype(BF16).astype(F32) + sent[k ^ bit].astype(F32) for k in held}
        else:
            held = {
                k: held[k].astype(BF16).astype(F32) + sent[k ^ bit].astype(F32)
                for k in held
                if not k & bit
            }
    return held


def head_norm(projected, gain):
    shaped = projected.reshape(projected.shape[0], -1, gain.shape[0])
    normed = shaped * lax.rsqrt(jnp.mean(shaped * shaped, axis=-1, keepdims=True) + epsilon) * gain
    return normed.astype(BF16)


def on_device(
    mesh_shape,
    latents,
    lengths,
    t_index,
    mod_scale,
    q_weight,
    k_weight,
    v_weight,
    out_weight,
    q_gain,
    k_gain,
    student_weight,
):
    n_seq, n_tp = mesh_shape["seq"], mesh_shape["tp"]
    row_count, width_here = latents.shape
    head_dim = q_gain.shape[0]
    heads_here = q_weight.shape[1] // head_dim
    tp_index = lax.axis_index("tp")
    seq_index = lax.axis_index("seq")
    image_ends = jnp.cumsum(lengths)
    score_scale = 1.0 / math.sqrt(head_dim)
    step_size = 1.0 / TGRID

    spread = math.gcd(heads_here, n_seq)
    groups = n_seq // spread
    heads_kept = heads_here // spread
    twisted = groups == 2 and spread >= 4
    group_index = seq_index // spread
    head_block = seq_index % spread
    if twisted:
        head_block = head_block ^ (group_index * 2)

    def rows_image(source):
        return image_index(source * row_count + jnp.arange(row_count, dtype=jnp.int32), image_ends)

    query_image = rows_image(seq_index)
    one_hot = (
        query_image[:, None] == jnp.arange(lengths.shape[0], dtype=jnp.int32)[None, :]
    ).astype(F32)
    start_times = jnp.sum(one_hot * (t_index.astype(F32) / TGRID)[None, :], axis=1)

    group_image = jnp.concatenate([rows_image(seq_index ^ m) for m in range(spread)])
    if groups == 2:
        partner_mask = spread ^ 2 if twisted else spread
        key_image = jnp.concatenate(
            [group_image] + [rows_image(seq_index ^ partner_mask ^ m) for m in range(spread)]
        )
    else:
        key_image = jnp.concatenate(
            [
                rows_image((seq_index % spread ^ m) + g * spread)
                for g in range(groups)
                for m in range(spread)
            ]
        )
    same_image = group_image[:, None] == key_image[None, :]

    def attention(queries, key_rows, value_rows):
        wide = heads_kept * head_dim
        packed = jnp.concatenate(
            [
                part.reshape(row_count, spread, 1, wide)
                for part in (queries, key_rows, value_rows)
            ],
            axis=2,
        )
        received = []
        for m in range(spread):
            piece = lax.dynamic_index_in_dim(packed, head_block ^ m, 1, keepdims=False)
            piece = piece.reshape(row_count, 3 * wide)
            received.append(piece if m == 0 else swap(piece, "seq", n_seq, m))
        own = jnp.concatenate(received, axis=0)
        group_q, group_kv = own[:, :wide], own[:, wide:]
        if groups == 2:
            other = swap(group_kv, "seq", n_seq, partner_mask)
            whole_kv = jnp.concatenate([group_kv, other], axis=0)
        elif groups == 1:
            whole_kv = group_kv
        else:
            whole_kv = lax.all_gather(
                group_kv,
                "seq",
                axis=0,
                tiled=True,
                axis_index_groups=[
                    [a + g * spread for g in range(groups)] for a in range(spread)
                ],
            )
        outs = []
        for h in range(heads_kept):
            cut = slice(h * head_dim, (h + 1) * head_dim)
            q_h, k_h = group_q[:, cut], whole_kv[:, :wide][:, cut]
            v_h = whole_kv[:, wide:][:, cut]
            scores = jnp.dot(q_h, k_h.T, preferred_element_type=F32) * score_scale
            scores = jnp.where(same_image, scores, -1e30)
            highest = jnp.max(scores, axis=1, keepdims=True)
            weights = jnp.where(same_image, jnp.exp(scores - highest), 0.0)
            totals = jnp.sum(weights, axis=1, keepdims=True)
            mixed = jnp.dot(weights.astype(BF16), v_h, preferred_element_type=F32)
            outs.append((mixed / totals).astype(BF16))
        result = jnp.concatenate(outs, axis=1) if len(outs) > 1 else outs[0]
        back = []
        for m in range(spread):
            piece = result[m * row_count : (m + 1) * row_count]
            back.append(piece if m == 0 else swap(piece, "seq", n_seq, m))
        return jnp.concatenate(in_order(back, head_block), axis=1)

    def terms_of(left, right):
        product = jnp.dot(left, right, preferred_element_type=F32)
        return [
            lax.dynamic_slice_in_dim(product, (tp_index ^ k) * width_here, width_here, 1)
            for k in range(n_tp)
        ]

    def teacher(state_blocks, times):
        state32 = jnp.concatenate(in_order(state_blocks, tp_index), axis=1).astype(F32)
        normed = state32 * lax.rsqrt(jnp.mean(state32 * state32, axis=1, keepdims=True) + epsilon)
        hidden = (normed * (1.0 + times[:, None] * mod_scale[None, :])).astype(BF16)
        queries = head_norm(jnp.dot(hidden, q_weight, preferred_element_type=F32), q_gain)
        key_rows = head_norm(jnp.dot(hidden, k_weight, preferred_element_type=F32), k_gain)
        value_rows = jnp.dot(hidden, v_weight, preferred_element_type=F32).astype(BF16)
        mixed = attention(queries, key_rows, value_rows)
        return terms_of(mixed, out_weight), hidden

    def step(block, velocity):
        return (block.astype(F32) + step_size * velocity.astype(F32)).astype(BF16)

    blocks = gather_blocks(latents, "tp", n_tp)
    terms, first_hidden = teacher(blocks, start_times)
    held = reduce_blocks(terms, "tp", n_tp, True)
    velocity0 = held[0].astype(BF16)
    moved = {k: step(blocks[k], held[k].astype(BF16)) for k in held}
    for bit in reversed(bits_of(n_tp)[:-1]):
        for k in list(moved):
            moved[k ^ bit] = swap(moved[k], "tp", n_tp, bit)
    terms, _ = teacher([moved[k] for k in range(n_tp)], start_times + step_size)
    velocity1 = reduce_blocks(terms, "tp", n_tp, False)[0].astype(BF16)

    columns = lax.dynamic_slice_in_dim(first_hidden, tp_index * width_here, width_here, 1)
    student = reduce_blocks(terms_of(columns, student_weight), "tp", n_tp, False)[0].astype(BF16)

    target = (0.5 * (velocity0.astype(F32) + velocity1.astype(F32))).astype(BF16)
    student32 = student.astype(F32)
    residual = student32 - target.astype(F32)
    per_token = jnp.sum(residual * residual, axis=1) + kinetic_weight * jnp.sum(
        student32 * student32, axis=1
    )
    image_sum = jnp.sum(one_hot * per_token[:, None], axis=0)
    for bit in bits_of(n_tp):
        image_sum = image_sum + swap(image_sum, "tp", n_tp, bit)
    for bit in bits_of(n_seq):
        image_sum = image_sum + swap(image_sum, "seq", n_seq, bit)
    loss = jnp.mean(image_sum / (lengths.astype(F32) * mod_scale.shape[0]))
    return (target, student, loss)


def solution(mesh):
    placed = (
        P("seq", "tp"),
        P(),
        P(),
        P(),
        P(None, "tp"),
        P(None, "tp"),
        P(None, "tp"),
        P("tp", None),
        P(),
        P(),
        P("tp", None),
    )

    def body(*arguments):
        return on_device(dict(mesh.shape), *arguments)

    return jax.shard_map(
        body,
        mesh=mesh,
        in_specs=placed,
        out_specs=(P("seq", "tp"), P("seq", "tp"), P()),
        check_vma=False,
    )
```

```python
import functools
import math

import jax
import jax.numpy as jnp
from jax import lax
from jax.experimental import pallas as pl
from jax.experimental.pallas import tpu as pltpu
from jax.sharding import PartitionSpec as P

TGRID = 8
epsilon = 1e-06
kinetic_weight = 0.1
F32, BF16 = jnp.float32, jnp.bfloat16
KERNEL_VMEM = 24 * 1024 * 1024


def image_index(positions, image_ends):
    return jnp.sum((positions[:, None] >= image_ends[None, :]).astype(jnp.int32), axis=1)


def swap(value, axis, size, mask):
    return lax.ppermute(value, axis, [(i, i ^ mask) for i in range(size)])


def bits_of(size):
    return [1 << b for b in range(size.bit_length() - 1)]


def gather_blocks(own, axis, size):
    blocks = {0: own}
    for bit in reversed(bits_of(size)):
        for k in list(blocks):
            blocks[k ^ bit] = swap(blocks[k], axis, size, bit)
    return [blocks[k] for k in range(size)]


def in_order(blocks, index):
    size = len(blocks)
    current = list(blocks)
    for bit in bits_of(size):
        flip = (index & bit) != 0
        current = [jnp.where(flip, current[k ^ bit], current[k]) for k in range(size)]
    return current


def reduce_blocks(terms, axis, size, keep_last):
    held = dict(enumerate(terms))
    bits = bits_of(size)
    for bit in bits:
        last = keep_last and bit == bits[-1]
        sent = {k: swap(held[k].astype(BF16), axis, size, bit) for k in held if last or k & bit}
        if last:
            held = {k: held[k].astype(BF16).astype(F32) + sent[k ^ bit].astype(F32) for k in held}
        else:
            held = {
                k: held[k].astype(BF16).astype(F32) + sent[k ^ bit].astype(F32)
                for k in held
                if not k & bit
            }
    return held


def head_norm(projected, gain):
    shaped = projected.reshape(projected.shape[0], -1, gain.shape[0])
    normed = shaped * lax.rsqrt(jnp.mean(shaped * shaped, axis=-1, keepdims=True) + epsilon) * gain
    return normed.astype(BF16)


def on_device(
    mesh_shape,
    latents,
    lengths,
    t_index,
    mod_scale,
    q_weight,
    k_weight,
    v_weight,
    out_weight,
    q_gain,
    k_gain,
    student_weight,
):
    n_seq, n_tp = mesh_shape["seq"], mesh_shape["tp"]
    row_count, width_here = latents.shape
    head_dim = q_gain.shape[0]
    heads_here = q_weight.shape[1] // head_dim
    tp_index = lax.axis_index("tp")
    seq_index = lax.axis_index("seq")
    image_ends = jnp.cumsum(lengths)
    score_scale = 1.0 / math.sqrt(head_dim)
    step_size = 1.0 / TGRID

    spread = math.gcd(heads_here, n_seq)
    groups = n_seq // spread
    heads_kept = heads_here // spread
    twisted = groups == 2 and spread >= 4
    group_index = seq_index // spread
    head_block = seq_index % spread
    if twisted:
        head_block = head_block ^ (group_index * 2)

    def rows_image(source):
        return image_index(source * row_count + jnp.arange(row_count, dtype=jnp.int32), image_ends)

    query_image = rows_image(seq_index)
    one_hot = (
        query_image[:, None] == jnp.arange(lengths.shape[0], dtype=jnp.int32)[None, :]
    ).astype(F32)
    start_times = jnp.sum(one_hot * (t_index.astype(F32) / TGRID)[None, :], axis=1)

    group_image = jnp.concatenate([rows_image(seq_index ^ m) for m in range(spread)])
    if groups == 2:
        partner_mask = spread ^ 2 if twisted else spread
        key_image = jnp.concatenate(
            [group_image] + [rows_image(seq_index ^ partner_mask ^ m) for m in range(spread)]
        )
    else:
        key_image = jnp.concatenate(
            [
                rows_image((seq_index % spread ^ m) + g * spread)
                for g in range(groups)
                for m in range(spread)
            ]
        )
    same_image = group_image[:, None] == key_image[None, :]

    def attention(queries, key_rows, value_rows):
        wide = heads_kept * head_dim
        packed = jnp.concatenate(
            [
                part.reshape(row_count, spread, 1, wide)
                for part in (queries, key_rows, value_rows)
            ],
            axis=2,
        )
        received = []
        for m in range(spread):
            piece = lax.dynamic_index_in_dim(packed, head_block ^ m, 1, keepdims=False)
            piece = piece.reshape(row_count, 3 * wide)
            received.append(piece if m == 0 else swap(piece, "seq", n_seq, m))
        own = jnp.concatenate(received, axis=0)
        group_q, group_kv = own[:, :wide], own[:, wide:]
        if groups == 2:
            other = swap(group_kv, "seq", n_seq, partner_mask)
            whole_kv = jnp.concatenate([group_kv, other], axis=0)
        elif groups == 1:
            whole_kv = group_kv
        else:
            whole_kv = lax.all_gather(
                group_kv,
                "seq",
                axis=0,
                tiled=True,
                axis_index_groups=[
                    [a + g * spread for g in range(groups)] for a in range(spread)
                ],
            )
        outs = []
        for h in range(heads_kept):
            cut = slice(h * head_dim, (h + 1) * head_dim)
            q_h, k_h = group_q[:, cut], whole_kv[:, :wide][:, cut]
            v_h = whole_kv[:, wide:][:, cut]
            scores = jnp.dot(q_h, k_h.T, preferred_element_type=F32) * score_scale
            scores = jnp.where(same_image, scores, -1e30)
            highest = jnp.max(scores, axis=1, keepdims=True)
            weights = jnp.where(same_image, jnp.exp(scores - highest), 0.0)
            totals = jnp.sum(weights, axis=1, keepdims=True)
            mixed = jnp.dot(weights.astype(BF16), v_h, preferred_element_type=F32)
            outs.append((mixed / totals).astype(BF16))
        result = jnp.concatenate(outs, axis=1) if len(outs) > 1 else outs[0]
        back = []
        for m in range(spread):
            piece = result[m * row_count : (m + 1) * row_count]
            back.append(piece if m == 0 else swap(piece, "seq", n_seq, m))
        return jnp.concatenate(in_order(back, head_block), axis=1)

    def terms_of(left, right):
        product = jnp.dot(left, right, preferred_element_type=F32)
        return [
            lax.dynamic_slice_in_dim(product, (tp_index ^ k) * width_here, width_here, 1)
            for k in range(n_tp)
        ]

    def teacher(state_blocks, times):
        state32 = jnp.concatenate(in_order(state_blocks, tp_index), axis=1).astype(F32)
        normed = state32 * lax.rsqrt(jnp.mean(state32 * state32, axis=1, keepdims=True) + epsilon)
        hidden = (normed * (1.0 + times[:, None] * mod_scale[None, :])).astype(BF16)
        queries = head_norm(jnp.dot(hidden, q_weight, preferred_element_type=F32), q_gain)
        key_rows = head_norm(jnp.dot(hidden, k_weight, preferred_element_type=F32), k_gain)
        value_rows = jnp.dot(hidden, v_weight, preferred_element_type=F32).astype(BF16)
        mixed = attention(queries, key_rows, value_rows)
        return terms_of(mixed, out_weight), hidden

    def step(block, velocity):
        return (block.astype(F32) + step_size * velocity.astype(F32)).astype(BF16)

    blocks = gather_blocks(latents, "tp", n_tp)
    terms, first_hidden = teacher(blocks, start_times)
    held = reduce_blocks(terms, "tp", n_tp, True)
    velocity0 = held[0].astype(BF16)
    moved = {k: step(blocks[k], held[k].astype(BF16)) for k in held}
    for bit in reversed(bits_of(n_tp)[:-1]):
        for k in list(moved):
            moved[k ^ bit] = swap(moved[k], "tp", n_tp, bit)
    terms, _ = teacher([moved[k] for k in range(n_tp)], start_times + step_size)
    velocity1 = reduce_blocks(terms, "tp", n_tp, False)[0].astype(BF16)

    columns = lax.dynamic_slice_in_dim(first_hidden, tp_index * width_here, width_here, 1)
    student = reduce_blocks(terms_of(columns, student_weight), "tp", n_tp, False)[0].astype(BF16)

    target = (0.5 * (velocity0.astype(F32) + velocity1.astype(F32))).astype(BF16)
    student32 = student.astype(F32)
    residual = student32 - target.astype(F32)
    per_token = jnp.sum(residual * residual, axis=1) + kinetic_weight * jnp.sum(
        student32 * student32, axis=1
    )
    image_sum = jnp.sum(one_hot * per_token[:, None], axis=0)
    for bit in bits_of(n_tp):
        image_sum = image_sum + swap(image_sum, "tp", n_tp, bit)
    for bit in bits_of(n_seq):
        image_sum = image_sum + swap(image_sum, "seq", n_seq, bit)
    loss = jnp.mean(image_sum / (lengths.astype(F32) * mod_scale.shape[0]))
    return (target, student, loss)


def whole(shape, dtype=BF16):
    return jax.ShapeDtypeStruct(shape, dtype)


VM = pl.BlockSpec(memory_space=pltpu.VMEM)


def call(body, outs, flops, *operands):
    size = sum(math.prod(a.shape) * a.dtype.itemsize for a in operands)
    return pl.pallas_call(
        body,
        out_shape=outs,
        in_specs=[VM] * len(operands),
        out_specs=jax.tree.map(lambda _: VM, outs),
        compiler_params=pltpu.CompilerParams(vmem_limit_bytes=KERNEL_VMEM),
        cost_estimate=pl.CostEstimate(flops=flops, bytes_accessed=size, transcendentals=0),
    )(*operands)


def head_at(block, m, width):
    return pl.ds(pl.multiple_of((block ^ m) * width, width), width)


def normed_head(raw, gain):
    return (raw * lax.rsqrt(jnp.mean(raw * raw, axis=1, keepdims=True) + epsilon) * gain).astype(
        BF16
    )


def head_block_of(spread, twisted):
    seq_index = lax.axis_index("seq")
    block = lax.rem(seq_index, spread)
    if twisted:
        block = block ^ (lax.div(seq_index, spread) * 2)
    return block


def kv_kernel(plan, moving, *refs):
    n_tp, _, spread, twisted, head_dim, step_size = plan
    state, refs = refs[:n_tp], refs[n_tp:]
    if moving:
        near, far, refs = refs[:n_tp], refs[n_tp : 2 * n_tp], refs[2 * n_tp :]
    time_ref, mod_ref, k_ref, v_ref, gain_ref, rows_ref, scale_ref = refs[:7]
    outs = refs[7:]
    tp_index = lax.axis_index("tp")
    block = head_block_of(spread, twisted)
    width = state[0].shape[1]
    times = time_ref[...]
    squares = jnp.zeros_like(times)
    for k in range(n_tp):
        x = state[k][...].astype(F32)
        if moving:
            velocity = (near[k][...].astype(F32) + far[k][...].astype(F32)).astype(BF16)
            x = (x + step_size * velocity.astype(F32)).astype(BF16).astype(F32)
        squares = squares + jnp.sum(x * x, axis=1, keepdims=True)
        mod = mod_ref[:, head_at(tp_index, k, width)]
        rows_ref[:, k * width : (k + 1) * width] = (x * (1.0 + times * mod)).astype(BF16)
    scale = lax.rsqrt(squares / (n_tp * width) + epsilon)
    scale_ref[...] = scale
    for m in range(spread):
        columns = head_at(block, m, head_dim)
        total = None
        for k in range(n_tp):
            rows = head_at(tp_index, k, width)
            weight = jnp.concatenate([k_ref[rows, columns], v_ref[rows, columns]], axis=1)
            part = jnp.dot(
                rows_ref[:, k * width : (k + 1) * width], weight, preferred_element_type=F32
            )
            total = part if total is None else total + part
        total = total * scale
        outs[m][:, :head_dim] = normed_head(total[:, :head_dim], gain_ref[...])
        outs[m][:, head_dim:] = total[:, head_dim:].astype(BF16)


def q_kernel(plan, rows_ref, scale_ref, q_ref, gain_ref, *outs):
    n_tp, _, spread, twisted, head_dim, _ = plan
    tp_index = lax.axis_index("tp")
    block = head_block_of(spread, twisted)
    width = rows_ref.shape[1] // n_tp
    for first in range(0, spread, 2):
        total = None
        for k in range(n_tp):
            rows = head_at(tp_index, k, width)
            weight = jnp.concatenate(
                [q_ref[rows, head_at(block, m, head_dim)] for m in (first, first + 1)], axis=1
            )
            part = jnp.dot(
                rows_ref[:, k * width : (k + 1) * width], weight, preferred_element_type=F32
            )
            total = part if total is None else total + part
        total = total * scale_ref[...]
        for m in range(2):
            cut = total[:, m * head_dim : (m + 1) * head_dim]
            outs[first + m][...] = normed_head(cut, gain_ref[...])


def terms_kernel(n_tp, left_ref, right_ref, scale_ref, *outs):
    tp_index = lax.axis_index("tp")
    width = outs[0].shape[1]
    for k in range(n_tp):
        product = jnp.dot(
            left_ref[...],
            right_ref[:, head_at(tp_index, k, width)],
            preferred_element_type=F32,
        )
        outs[k][...] = (product * scale_ref[...]).astype(BF16)


def out_kernel(plan, *refs):
    n_tp, _, spread, twisted, head_dim, _ = plan
    pieces, right_ref, outs = refs[:spread], refs[spread], refs[spread + 1 :]
    tp_index = lax.axis_index("tp")
    block = head_block_of(spread, twisted)
    width = outs[0].shape[1]
    left = jnp.concatenate([piece[...] for piece in pieces], axis=1)
    for k in list(range(1, n_tp, 2)) + list(range(0, n_tp, 2)):
        columns = head_at(tp_index, k, width)
        right = jnp.concatenate(
            [right_ref[head_at(block, m, head_dim), columns] for m in range(spread)], axis=0
        )
        outs[k][...] = jnp.dot(left, right, preferred_element_type=F32).astype(BF16)


def scores_of(query, keys, query_image, key_image, head_dim):
    scores = lax.dot_general(
        query, keys, (((1,), (1,)), ((), ())), preferred_element_type=F32
    ) * (1.0 / math.sqrt(head_dim))
    return jnp.where(query_image == key_image, scores, -1e30)


def near_kernel(spread, head_dim, *refs):
    queries, pairs, refs = refs[:spread], refs[spread : 2 * spread], refs[2 * spread :]
    query_image, key_image, top_ref, total_ref, sum_ref = refs
    rows = queries[0].shape[0]
    keys = jnp.concatenate([pair[:, :head_dim] for pair in pairs], axis=0)
    values = jnp.concatenate([pair[:, head_dim:] for pair in pairs], axis=0)
    for m in range(spread):
        cut = slice(m * rows, (m + 1) * rows)
        scores = scores_of(queries[m][...], keys, query_image[cut], key_image[...], head_dim)
        top = jnp.max(scores, axis=1, keepdims=True)
        weights = jnp.exp(scores - top)
        top_ref[cut] = top
        total_ref[cut] = jnp.sum(weights, axis=1, keepdims=True)
        sum_ref[cut] = jnp.dot(weights.astype(BF16), values, preferred_element_type=F32)


def far_kernel(spread, head_dim, *refs):
    queries, pairs, refs = refs[:spread], refs[spread : 2 * spread], refs[2 * spread :]
    query_image, key_image, top_ref, total_ref, sum_ref = refs[:5]
    outs = refs[5:]
    rows = queries[0].shape[0]
    keys = jnp.concatenate([pair[:, :head_dim] for pair in pairs], axis=0)
    values = jnp.concatenate([pair[:, head_dim:] for pair in pairs], axis=0)
    for m in range(spread):
        cut = slice(m * rows, (m + 1) * rows)
        scores = scores_of(queries[m][...], keys, query_image[cut], key_image[...], head_dim)
        old = top_ref[cut]
        top = jnp.maximum(old, jnp.max(scores, axis=1, keepdims=True))
        weights = jnp.exp(scores - top)
        fade = jnp.exp(old - top)
        total = total_ref[cut] * fade + jnp.sum(weights, axis=1, keepdims=True)
        mixed = sum_ref[cut] * fade + jnp.dot(
            weights.astype(BF16), values, preferred_element_type=F32
        )
        outs[m][...] = (mixed / total).astype(BF16)


def loss_kernel(*refs):
    near0, far0, near1, far1, student_ref, image_ref, target_ref, part_ref = refs
    velocity0 = (near0[...].astype(F32) + far0[...].astype(F32)).astype(BF16).astype(F32)
    velocity1 = (near1[...].astype(F32) + far1[...].astype(F32)).astype(BF16).astype(F32)
    target = (0.5 * (velocity0 + velocity1)).astype(BF16)
    target_ref[...] = target
    student = student_ref[...].astype(F32)
    residual = student - target.astype(F32)
    per_token = jnp.sum(residual * residual + kinetic_weight * (student * student), axis=1, keepdims=True)
    lanes = lax.broadcasted_iota(jnp.int32, part_ref.shape, 1)
    part_ref[...] = jnp.sum(
        jnp.where(image_ref[...] == lanes[:1], per_token, 0.0), axis=0, keepdims=True
    ) + jnp.zeros(part_ref.shape, F32)


def on_device_fused(
    mesh_shape,
    latents,
    lengths,
    t_index,
    mod_scale,
    q_weight,
    k_weight,
    v_weight,
    out_weight,
    q_gain,
    k_gain,
    student_weight,
):
    n_seq, n_tp = mesh_shape["seq"], mesh_shape["tp"]
    row_count, width = latents.shape
    head_dim = q_gain.shape[0]
    heads_here = q_weight.shape[1] // head_dim
    seq_index = lax.axis_index("seq")
    inner = n_tp * width
    step_size = 1.0 / TGRID
    spread = heads_here
    twisted = spread >= 4
    partner = spread ^ 2 if twisted else spread
    plan = (n_tp, n_seq, spread, twisted, head_dim, step_size)

    ends = [lengths[0]]
    for i in range(1, lengths.shape[0]):
        ends.append(ends[-1] + lengths[i])
    row = jnp.arange(row_count, dtype=jnp.int32)
    groups = jnp.arange(spread, dtype=jnp.int32)

    def images_of(sources):
        positions = (sources[:, None] * row_count + row[None, :]).reshape(-1)
        return sum((positions >= end).astype(jnp.int32) for end in ends)

    near_image = images_of(seq_index ^ groups)
    far_image = images_of(seq_index ^ partner ^ groups)
    own_image = images_of(seq_index[None])
    start_time = sum(
        jnp.where(own_image == i, t_index[i].astype(F32) / TGRID, 0.0)
        for i in range(lengths.shape[0])
    )[:, None]
    near_rows, near_keys, far_keys = near_image[:, None], near_image[None, :], far_image[None, :]
    own_rows = own_image[:, None]
    mod_row = mod_scale[None, :]
    q_row, k_row = q_gain[None, :], k_gain[None, :]

    def tp_swap(value, mask):
        return swap(value, "tp", n_tp, mask)

    def seq_swap(value, mask):
        return swap(value, "seq", n_seq, mask)

    def mixed_terms(state, velocity, times):
        operands = list(state)
        if velocity is not None:
            operands += velocity[0] + velocity[1]
        rows, scale, *pairs = call(
            functools.partial(kv_kernel, plan, velocity is not None),
            [whole((row_count, inner)), whole((row_count, 1), F32)]
            + [whole((row_count, 2 * head_dim))] * spread,
            4 * row_count * inner * spread * head_dim,
            *operands, times, mod_row, k_weight, v_weight, k_row,
        )
        near, far = [pairs[0]], [seq_swap(pairs[0], partner)]
        for m in range(1, spread):
            near.append(seq_swap(pairs[m], m))
        for m in range(1, spread):
            far.append(seq_swap(near[m], partner))
        queries = call(
            functools.partial(q_kernel, plan),
            [whole((row_count, head_dim))] * spread,
            2 * row_count * inner * spread * head_dim,
            rows, scale, q_weight, q_row,
        )
        queries = [queries[0]] + [seq_swap(queries[m], m) for m in range(1, spread)]
        flops = 4 * (spread * row_count) ** 2 * head_dim
        state3 = call(
            functools.partial(near_kernel, spread, head_dim),
            [whole((spread * row_count, 1), F32)] * 2
            + [whole((spread * row_count, head_dim), F32)],
            flops,
            *queries, *near, near_rows, near_keys,
        )
        pieces = call(
            functools.partial(far_kernel, spread, head_dim),
            [whole((row_count, head_dim))] * spread,
            flops,
            *queries, *far, near_rows, far_keys, *state3,
        )
        pieces = [pieces[0]] + [seq_swap(pieces[m], m) for m in range(1, spread)]
        terms = call(
            functools.partial(out_kernel, plan),
            [whole((row_count, width))] * n_tp,
            2 * row_count * spread * head_dim * inner,
            *pieces, out_weight,
        )
        return terms, rows, scale

    def halve(terms):
        held = dict(enumerate(terms))
        for bit in bits_of(n_tp)[:-1]:
            sent = {k: tp_swap(held[k], bit) for k in held if k & bit}
            held = {
                k: (held[k].astype(F32) + sent[k ^ bit].astype(F32)).astype(BF16)
                for k in held
                if not k & bit
            }
        return held

    def spread_low(held):
        held = dict(held)
        for bit in reversed(bits_of(n_tp)[:-1]):
            for k in list(held):
                held[k ^ bit] = tp_swap(held[k], bit)
        return [held[k] for k in range(n_tp)]

    top_bit = n_tp // 2
    blocks = gather_blocks(latents, "tp", n_tp)
    terms, rows, scale = mixed_terms(blocks, None, start_time)

    student_terms = call(
        functools.partial(terms_kernel, n_tp),
        [whole((row_count, width))] * n_tp,
        2 * row_count * width * inner,
        rows[:, :width], student_weight, scale,
    )
    held_s = halve(student_terms)
    student = (held_s[0].astype(F32) + tp_swap(held_s[top_bit], top_bit).astype(F32)).astype(BF16)

    held = halve(terms)
    other = {k ^ top_bit: tp_swap(held[k], top_bit) for k in sorted(held, reverse=True)}
    near_blocks, far_blocks = spread_low(held), spread_low(other)
    terms, _, _ = mixed_terms(blocks, (near_blocks, far_blocks), start_time + step_size)
    held1 = halve(terms)
    other1 = tp_swap(held1[top_bit], top_bit)
    target, part = call(
        loss_kernel,
        [whole((row_count, width)), whole((8, 128), F32)],
        10 * row_count * width,
        held[0], other[0], held1[0], other1, student, own_rows,
    )
    part = part + tp_swap(part, 1)
    for bit in bits_of(n_tp)[1:-1]:
        part = part + tp_swap(part, bit)

    def both(value, seq_mask, tp_mask):
        return lax.ppermute(
            value,
            ("seq", "tp"),
            [
                (s * n_tp + t, (s ^ seq_mask) * n_tp + (t ^ tp_mask))
                for s in range(n_seq)
                for t in range(n_tp)
            ],
        )

    part = (part + both(part, 0, top_bit)) + (both(part, 1, 0) + both(part, 1, top_bit))
    low = n_seq // 4
    part = (part + seq_swap(part, low)) + (seq_swap(part, 2 * low) + seq_swap(part, 3 * low))
    image_sum = part[0, : lengths.shape[0]]
    loss = jnp.mean(image_sum / (lengths.astype(F32) * inner))
    return (target, student, loss)


def solution(mesh):
    placed = (
        P("seq", "tp"),
        P(),
        P(),
        P(),
        P(None, "tp"),
        P(None, "tp"),
        P(None, "tp"),
        P("tp", None),
        P(),
        P(),
        P("tp", None),
    )

    def body(*arguments):
        latents, q_weight, q_gain = arguments[0], arguments[4], arguments[8]
        n_seq, n_tp = mesh.shape["seq"], mesh.shape["tp"]
        heads_here = q_weight.shape[1] // q_gain.shape[0]
        fused = (
            latents.shape[1] % 128 == 0
            and q_gain.shape[0] == 128
            and n_seq == 2 * heads_here == 8
            and n_tp in (2, 4)
        )
        run = on_device_fused if fused else on_device
        return run(dict(mesh.shape), *arguments)

    return jax.shard_map(
        body,
        mesh=mesh,
        in_specs=placed,
        out_specs=(P("seq", "tp"), P("seq", "tp"), P()),
        check_vma=False,
    )
```

```python
import functools
import math

import jax
import jax.numpy as jnp
from jax import lax
from jax.experimental import pallas as pl
from jax.experimental.pallas import tpu as pltpu
from jax.sharding import PartitionSpec as P


TGRID = 8
epsilon = 1e-06
kinetic_weight = 0.1
F32, BF16 = jnp.float32, jnp.bfloat16
KERNEL_VMEM = 16 * 1024 * 1024


def image_index(positions, image_ends):
    return jnp.sum((positions[:, None] >= image_ends[None, :]).astype(jnp.int32), axis=1)


def swap(value, axis, size, mask):
    return lax.ppermute(value, axis, [(i, i ^ mask) for i in range(size)])


def bits_of(size):
    return [1 << b for b in range(size.bit_length() - 1)]


def gather_blocks(own, axis, size):
    blocks = {0: own}
    for bit in reversed(bits_of(size)):
        for k in list(blocks):
            blocks[k ^ bit] = swap(blocks[k], axis, size, bit)
    return [blocks[k] for k in range(size)]


def in_order(blocks, index):
    size = len(blocks)
    current = list(blocks)
    for bit in bits_of(size):
        flip = (index & bit) != 0
        current = [jnp.where(flip, current[k ^ bit], current[k]) for k in range(size)]
    return current


def reduce_blocks(terms, axis, size, keep_last):
    held = dict(enumerate(terms))
    bits = bits_of(size)
    for bit in bits:
        last = keep_last and bit == bits[-1]
        sent = {k: swap(held[k].astype(BF16), axis, size, bit) for k in held if last or k & bit}
        if last:
            held = {k: held[k].astype(BF16).astype(F32) + sent[k ^ bit].astype(F32) for k in held}
        else:
            held = {
                k: held[k].astype(BF16).astype(F32) + sent[k ^ bit].astype(F32)
                for k in held
                if not k & bit
            }
    return held


def head_norm(projected, gain):
    shaped = projected.reshape(projected.shape[0], -1, gain.shape[0])
    normed = shaped * lax.rsqrt(jnp.mean(shaped * shaped, axis=-1, keepdims=True) + epsilon) * gain
    return normed.astype(BF16)


def on_device(
    mesh_shape,
    latents,
    lengths,
    t_index,
    mod_scale,
    q_weight,
    k_weight,
    v_weight,
    out_weight,
    q_gain,
    k_gain,
    student_weight,
):
    n_seq, n_tp = mesh_shape["seq"], mesh_shape["tp"]
    row_count, width_here = latents.shape
    head_dim = q_gain.shape[0]
    heads_here = q_weight.shape[1] // head_dim
    tp_index = lax.axis_index("tp")
    seq_index = lax.axis_index("seq")
    image_ends = jnp.cumsum(lengths)
    score_scale = 1.0 / math.sqrt(head_dim)
    step_size = 1.0 / TGRID

    spread = math.gcd(heads_here, n_seq)
    groups = n_seq // spread
    heads_kept = heads_here // spread
    twisted = groups == 2 and spread >= 4
    group_index = seq_index // spread
    head_block = seq_index % spread
    if twisted:
        head_block = head_block ^ (group_index * 2)

    def rows_image(source):
        return image_index(source * row_count + jnp.arange(row_count, dtype=jnp.int32), image_ends)

    query_image = rows_image(seq_index)
    one_hot = (
        query_image[:, None] == jnp.arange(lengths.shape[0], dtype=jnp.int32)[None, :]
    ).astype(F32)
    start_times = jnp.sum(one_hot * (t_index.astype(F32) / TGRID)[None, :], axis=1)

    group_image = jnp.concatenate([rows_image(seq_index ^ m) for m in range(spread)])
    if groups == 2:
        partner_mask = spread ^ 2 if twisted else spread
        key_image = jnp.concatenate(
            [group_image] + [rows_image(seq_index ^ partner_mask ^ m) for m in range(spread)]
        )
    else:
        key_image = jnp.concatenate(
            [
                rows_image((seq_index % spread ^ m) + g * spread)
                for g in range(groups)
                for m in range(spread)
            ]
        )
    same_image = group_image[:, None] == key_image[None, :]

    def attention(queries, key_rows, value_rows):
        wide = heads_kept * head_dim
        packed = jnp.concatenate(
            [
                part.reshape(row_count, spread, 1, wide)
                for part in (queries, key_rows, value_rows)
            ],
            axis=2,
        )
        received = []
        for m in range(spread):
            piece = lax.dynamic_index_in_dim(packed, head_block ^ m, 1, keepdims=False)
            piece = piece.reshape(row_count, 3 * wide)
            received.append(piece if m == 0 else swap(piece, "seq", n_seq, m))
        own = jnp.concatenate(received, axis=0)
        group_q, group_kv = own[:, :wide], own[:, wide:]
        if groups == 2:
            other = swap(group_kv, "seq", n_seq, partner_mask)
            whole_kv = jnp.concatenate([group_kv, other], axis=0)
        elif groups == 1:
            whole_kv = group_kv
        else:
            whole_kv = lax.all_gather(
                group_kv,
                "seq",
                axis=0,
                tiled=True,
                axis_index_groups=[
                    [a + g * spread for g in range(groups)] for a in range(spread)
                ],
            )
        outs = []
        for h in range(heads_kept):
            cut = slice(h * head_dim, (h + 1) * head_dim)
            q_h, k_h = group_q[:, cut], whole_kv[:, :wide][:, cut]
            v_h = whole_kv[:, wide:][:, cut]
            scores = jnp.dot(q_h, k_h.T, preferred_element_type=F32) * score_scale
            scores = jnp.where(same_image, scores, -1e30)
            highest = jnp.max(scores, axis=1, keepdims=True)
            weights = jnp.where(same_image, jnp.exp(scores - highest), 0.0)
            totals = jnp.sum(weights, axis=1, keepdims=True)
            mixed = jnp.dot(weights.astype(BF16), v_h, preferred_element_type=F32)
            outs.append((mixed / totals).astype(BF16))
        result = jnp.concatenate(outs, axis=1) if len(outs) > 1 else outs[0]
        back = []
        for m in range(spread):
            piece = result[m * row_count : (m + 1) * row_count]
            back.append(piece if m == 0 else swap(piece, "seq", n_seq, m))
        return jnp.concatenate(in_order(back, head_block), axis=1)

    def terms_of(left, right):
        product = jnp.dot(left, right, preferred_element_type=F32)
        return [
            lax.dynamic_slice_in_dim(product, (tp_index ^ k) * width_here, width_here, 1)
            for k in range(n_tp)
        ]

    def teacher(state_blocks, times):
        state32 = jnp.concatenate(in_order(state_blocks, tp_index), axis=1).astype(F32)
        normed = state32 * lax.rsqrt(jnp.mean(state32 * state32, axis=1, keepdims=True) + epsilon)
        hidden = (normed * (1.0 + times[:, None] * mod_scale[None, :])).astype(BF16)
        queries = head_norm(jnp.dot(hidden, q_weight, preferred_element_type=F32), q_gain)
        key_rows = head_norm(jnp.dot(hidden, k_weight, preferred_element_type=F32), k_gain)
        value_rows = jnp.dot(hidden, v_weight, preferred_element_type=F32).astype(BF16)
        mixed = attention(queries, key_rows, value_rows)
        return terms_of(mixed, out_weight), hidden

    def step(block, velocity):
        return (block.astype(F32) + step_size * velocity.astype(F32)).astype(BF16)

    blocks = gather_blocks(latents, "tp", n_tp)
    terms, first_hidden = teacher(blocks, start_times)
    held = reduce_blocks(terms, "tp", n_tp, True)
    velocity0 = held[0].astype(BF16)
    moved = {k: step(blocks[k], held[k].astype(BF16)) for k in held}
    for bit in reversed(bits_of(n_tp)[:-1]):
        for k in list(moved):
            moved[k ^ bit] = swap(moved[k], "tp", n_tp, bit)
    terms, _ = teacher([moved[k] for k in range(n_tp)], start_times + step_size)
    velocity1 = reduce_blocks(terms, "tp", n_tp, False)[0].astype(BF16)

    columns = lax.dynamic_slice_in_dim(first_hidden, tp_index * width_here, width_here, 1)
    student = reduce_blocks(terms_of(columns, student_weight), "tp", n_tp, False)[0].astype(BF16)

    target = (0.5 * (velocity0.astype(F32) + velocity1.astype(F32))).astype(BF16)
    student32 = student.astype(F32)
    residual = student32 - target.astype(F32)
    per_token = jnp.sum(residual * residual, axis=1) + kinetic_weight * jnp.sum(
        student32 * student32, axis=1
    )
    image_sum = jnp.sum(one_hot * per_token[:, None], axis=0)
    for bit in bits_of(n_tp):
        image_sum = image_sum + swap(image_sum, "tp", n_tp, bit)
    for bit in bits_of(n_seq):
        image_sum = image_sum + swap(image_sum, "seq", n_seq, bit)
    loss = jnp.mean(image_sum / (lengths.astype(F32) * mod_scale.shape[0]))
    return (target, student, loss)


def whole(shape, dtype=BF16):
    return jax.ShapeDtypeStruct(shape, dtype)


VM = pl.BlockSpec(memory_space=pltpu.VMEM)


def call(body, outs, flops, *operands, specs=None):
    size = sum(math.prod(a.shape) * a.dtype.itemsize for a in operands)
    return pl.pallas_call(
        body,
        out_shape=outs,
        in_specs=specs or [VM] * len(operands),
        out_specs=jax.tree.map(lambda _: VM, outs),
        compiler_params=pltpu.CompilerParams(vmem_limit_bytes=KERNEL_VMEM),
        cost_estimate=pl.CostEstimate(flops=flops, bytes_accessed=size, transcendentals=0),
    )(*operands)


def head_at(block, m, width):
    return pl.ds(pl.multiple_of((block ^ m) * width, width), width)


def normed_head(raw, gain):
    return (raw * lax.rsqrt(jnp.mean(raw * raw, axis=1, keepdims=True) + epsilon) * gain).astype(
        BF16
    )


def head_block_of(spread):
    return lax.rem(lax.axis_index("seq"), spread)


def fetch_kernel(count, *refs):
    sources, targets, sems = refs[:count], refs[count : 2 * count], refs[2 * count]
    copies = [
        pltpu.make_async_copy(source, target, sems.at[i])
        for i, (source, target) in enumerate(zip(sources, targets))
    ]
    for copy in copies:
        copy.start()
    for copy in copies:
        copy.wait()


def fetch(*arrays):
    count = len(arrays)
    size = sum(math.prod(a.shape) * a.dtype.itemsize for a in arrays)
    return pl.pallas_call(
        functools.partial(fetch_kernel, count),
        out_shape=[whole(a.shape, a.dtype) for a in arrays],
        in_specs=[pl.BlockSpec(memory_space=pltpu.HBM)] * count,
        out_specs=[VM] * count,
        scratch_shapes=[pltpu.SemaphoreType.DMA((count,))],
        compiler_params=pltpu.CompilerParams(vmem_limit_bytes=KERNEL_VMEM),
        cost_estimate=pl.CostEstimate(flops=200 * size, bytes_accessed=size, transcendentals=0),
    )(*[pltpu.with_memory_space_constraint(a, pltpu.HBM) for a in arrays])


def setup_kernel(partner, row_count, *refs):
    length_ref, index_ref, near_rows, near_keys, far_keys, own_rows, time_ref = refs
    seq_index = lax.axis_index("seq")
    images = length_ref.shape[0]
    ends = [length_ref[0]]
    for i in range(1, images):
        ends.append(ends[-1] + length_ref[i])

    def image_of(shape, axis, source):
        places = lax.broadcasted_iota(jnp.int32, shape, axis)
        blocks = lax.div(places, row_count)
        places = ((source ^ blocks) - blocks) * row_count + places
        return sum((places >= end).astype(jnp.int32) for end in ends)

    near_rows[...] = image_of(near_rows.shape, 0, seq_index)
    near_keys[...] = image_of(near_keys.shape, 1, seq_index)
    far_keys[...] = image_of(far_keys.shape, 1, seq_index ^ partner)
    own = image_of(own_rows.shape, 0, seq_index)
    own_rows[...] = own
    time = jnp.zeros(own.shape, F32)
    for i in range(images):
        time = jnp.where(own == i, index_ref[i].astype(F32) / TGRID, time)
    time_ref[...] = time


def qkv_kernel(plan, moving, *refs):
    n_tp, _, spread, head_dim, step_size = plan
    state, refs = refs[:n_tp], refs[n_tp:]
    if moving:
        near, far, refs = refs[:n_tp], refs[n_tp : 2 * n_tp], refs[2 * n_tp :]
    time_ref, mod_ref, q_ref, k_ref, v_ref, q_gain, k_gain, rows_ref, scale_ref = refs[:9]
    outs, pairs = refs[9 : 9 + spread], refs[9 + spread :]
    tp_index = lax.axis_index("tp")
    block = head_block_of(spread)
    width = state[0].shape[1]
    times = time_ref[...]
    if moving:
        times = times + step_size
    squares = jnp.zeros_like(times)
    for k in range(n_tp):
        x = state[k][...].astype(F32)
        if moving:
            velocity = (near[k][...].astype(F32) + far[k][...].astype(F32)).astype(BF16)
            x = (x + step_size * velocity.astype(F32)).astype(BF16).astype(F32)
        squares = squares + jnp.sum(x * x, axis=1, keepdims=True)
        mod = mod_ref[:, head_at(tp_index, k, width)]
        rows_ref[:, k * width : (k + 1) * width] = (x * (1.0 + times * mod)).astype(BF16)
    scale = lax.rsqrt(squares / (n_tp * width) + epsilon)
    scale_ref[...] = scale

    def project(pieces):
        total = None
        for k in range(n_tp):
            rows = head_at(tp_index, k, width)
            weight = jnp.concatenate(
                [ref[rows, head_at(block, m, head_dim)] for ref, m in pieces], axis=1
            )
            part = jnp.dot(
                rows_ref[:, k * width : (k + 1) * width], weight, preferred_element_type=F32
            )
            total = part if total is None else total + part
        return total * scale

    for m in [*range(1, spread), 0]:
        total = project([(k_ref, m), (v_ref, m)])
        keys = normed_head(total[:, :head_dim], k_gain[...])
        values = total[:, head_dim:].astype(BF16)
        outs[m][:, head_dim : 2 * head_dim] = keys
        outs[m][:, 2 * head_dim :] = values
        pairs[m][:, :head_dim] = keys
        pairs[m][:, head_dim:] = values
    for first in range(0, spread, 2):
        total = project([(q_ref, first), (q_ref, first + 1)])
        for m in range(2):
            cut = total[:, m * head_dim : (m + 1) * head_dim]
            outs[first + m][:, :head_dim] = normed_head(cut, q_gain[...])


def terms_kernel(n_tp, left_ref, right_ref, scale_ref, *outs):
    tp_index = lax.axis_index("tp")
    width = outs[0].shape[1]
    for k in range(n_tp):
        product = jnp.dot(
            left_ref[:, :width],
            right_ref[:, head_at(tp_index, k, width)],
            preferred_element_type=F32,
        )
        outs[k][...] = (product * scale_ref[...]).astype(BF16)


def add_kernel(count, *refs):
    for own, other, out in zip(refs[:count], refs[count : 2 * count], refs[2 * count :]):
        out[...] = (own[...].astype(F32) + other[...].astype(F32)).astype(BF16)


def out_kernel(plan, *refs):
    n_tp, _, spread, head_dim, _ = plan
    pieces, right_ref, outs = refs[:spread], refs[spread], refs[spread + 1 :]
    tp_index = lax.axis_index("tp")
    block = head_block_of(spread)
    width = outs[0].shape[1]
    left = jnp.concatenate([piece[...] for piece in pieces], axis=1)
    for k in list(range(1, n_tp, 2)) + list(range(0, n_tp, 2)):
        columns = head_at(tp_index, k, width)
        right = jnp.concatenate(
            [right_ref[head_at(block, m, head_dim), columns] for m in range(spread)], axis=0
        )
        outs[k][...] = jnp.dot(left, right, preferred_element_type=F32).astype(BF16)


def scores_of(query, keys, query_image, key_image, head_dim):
    scores = lax.dot_general(
        query, keys, (((1,), (1,)), ((), ())), preferred_element_type=F32
    ) * (1.0 / math.sqrt(head_dim))
    return jnp.where(query_image == key_image, scores, -1e30)


def near_kernel(spread, head_dim, *refs):
    triples, refs = refs[:spread], refs[spread:]
    query_image, key_image, top_ref, total_ref, sum_ref = refs
    rows = triples[0].shape[0]
    keys = jnp.concatenate([triple[:, head_dim : 2 * head_dim] for triple in triples], axis=0)
    values = jnp.concatenate([triple[:, 2 * head_dim :] for triple in triples], axis=0)
    for m in range(spread):
        cut = slice(m * rows, (m + 1) * rows)
        scores = scores_of(
            triples[m][:, :head_dim], keys, query_image[cut], key_image[...], head_dim
        )
        top = jnp.max(scores, axis=1, keepdims=True)
        weights = jnp.exp(scores - top)
        top_ref[cut] = top
        total_ref[cut] = jnp.sum(weights, axis=1, keepdims=True)
        sum_ref[cut] = jnp.dot(weights.astype(BF16), values, preferred_element_type=F32)


def far_kernel(spread, head_dim, *refs):
    triples, pairs, refs = refs[:spread], refs[spread : 2 * spread], refs[2 * spread :]
    query_image, key_image, top_ref, total_ref, sum_ref = refs[:5]
    outs = refs[5:]
    rows = triples[0].shape[0]
    keys = jnp.concatenate([pair[:, :head_dim] for pair in pairs], axis=0)
    values = jnp.concatenate([pair[:, head_dim:] for pair in pairs], axis=0)
    for m in [*range(1, spread), 0]:
        cut = slice(m * rows, (m + 1) * rows)
        scores = scores_of(
            triples[m][:, :head_dim], keys, query_image[cut], key_image[...], head_dim
        )
        old = top_ref[cut]
        top = jnp.maximum(old, jnp.max(scores, axis=1, keepdims=True))
        weights = jnp.exp(scores - top)
        fade = jnp.exp(old - top)
        total = total_ref[cut] * fade + jnp.sum(weights, axis=1, keepdims=True)
        mixed = sum_ref[cut] * fade + jnp.dot(
            weights.astype(BF16), values, preferred_element_type=F32
        )
        outs[m][...] = (mixed / total).astype(BF16)


def loss_kernel(*refs):
    near0, far0, near1, far1, student_ref, image_ref, target_ref, part_ref = refs
    velocity0 = (near0[...].astype(F32) + far0[...].astype(F32)).astype(BF16).astype(F32)
    velocity1 = (near1[...].astype(F32) + far1[...].astype(F32)).astype(BF16).astype(F32)
    target = (0.5 * (velocity0 + velocity1)).astype(BF16)
    target_ref[...] = target
    student = student_ref[...].astype(F32)
    residual = student - target.astype(F32)
    per_token = jnp.sum(residual * residual + kinetic_weight * (student * student), axis=1, keepdims=True)
    lanes = lax.broadcasted_iota(jnp.int32, part_ref.shape, 1)
    part_ref[...] = jnp.sum(
        jnp.where(image_ref[...] == lanes[:1], per_token, 0.0), axis=0, keepdims=True
    ) + jnp.zeros(part_ref.shape, F32)


def on_device_fused(
    mesh_shape,
    latents,
    lengths,
    t_index,
    mod_scale,
    q_weight,
    k_weight,
    v_weight,
    out_weight,
    q_gain,
    k_gain,
    student_weight,
):
    n_seq, n_tp = mesh_shape["seq"], mesh_shape["tp"]
    row_count, width = latents.shape
    head_dim = q_gain.shape[0]
    heads_here = q_weight.shape[1] // head_dim
    inner = n_tp * width
    step_size = 1.0 / TGRID
    spread = heads_here
    plan = (n_tp, n_seq, spread, head_dim, step_size)

    grouped = spread * row_count
    mod_row = mod_scale[None, :]
    q_row, k_row = q_gain[None, :], k_gain[None, :]

    def tp_swap(value, mask):
        return swap(value, "tp", n_tp, mask)

    def seq_swap(value, mask):
        return swap(value, "seq", n_seq, mask)

    def project(state, velocity, times):
        operands = list(state)
        if velocity is not None:
            operands += velocity[0] + velocity[1]
        rows, scale, *blocks = call(
            functools.partial(qkv_kernel, plan, velocity is not None),
            [whole((row_count, inner)), whole((row_count, 1), F32)]
            + [whole((row_count, 3 * head_dim))] * spread
            + [whole((row_count, 2 * head_dim))] * spread,
            6 * row_count * inner * spread * head_dim,
            *operands, times, mod_row, q_weight, k_weight, v_weight, q_row, k_row,
        )
        return rows, scale, blocks[:spread], blocks[spread:]

    def attend(triples, pairs):
        far_pairs, near_triples = [], [triples[0]]
        for m in range(spread):
            far_pairs.append(seq_swap(pairs[m], spread ^ m))
        for m in range(1, spread):
            near_triples.append(seq_swap(triples[m], m))
        flops = 4 * grouped**2 * head_dim
        sums = call(
            functools.partial(near_kernel, spread, head_dim),
            [whole((grouped, 1), F32)] * 2 + [whole((grouped, head_dim), F32)],
            flops,
            *near_triples, near_rows, near_keys,
        )
        pieces = call(
            functools.partial(far_kernel, spread, head_dim),
            [whole((row_count, head_dim))] * spread,
            flops,
            *near_triples, *far_pairs, near_rows, far_keys, *sums,
        )
        back = [pieces[0]]
        for m in range(1, spread):
            back.append(seq_swap(pieces[m], m))
        return call(
            functools.partial(out_kernel, plan),
            [whole((row_count, width))] * n_tp,
            2 * row_count * spread * head_dim * inner,
            *back, out_weight,
        )

    def halve(terms):
        held = dict(enumerate(terms))
        for bit in bits_of(n_tp)[:-1]:
            sent = {k: tp_swap(held[k], bit) for k in held if k & bit}
            kept = [k for k in held if not k & bit]
            sums = call(
                functools.partial(add_kernel, len(kept)),
                [whole((row_count, width))] * len(kept),
                1000 * row_count,
                *[held[k] for k in kept], *[sent[k ^ bit] for k in kept],
            )
            held = dict(zip(kept, sums))
        return held

    def spread_low(held):
        held = dict(held)
        for bit in reversed(bits_of(n_tp)[:-1]):
            for k in list(held):
                held[k ^ bit] = tp_swap(held[k], bit)
        return held

    top_bit = n_tp // 2
    top_block = tp_swap(latents, top_bit)
    held = spread_low({0: latents}) | spread_low({top_bit: top_block})
    blocks = [held[k] for k in range(n_tp)]
    blocks[0], q_weight, k_weight, v_weight, mod_row, q_row, k_row = fetch(
        latents, q_weight, k_weight, v_weight, mod_row, q_row, k_row
    )
    near_rows, near_keys, far_keys, own_rows, start_time = call(
        functools.partial(setup_kernel, spread, row_count),
        [
            whole((grouped, 1), jnp.int32),
            whole((1, grouped), jnp.int32),
            whole((1, grouped), jnp.int32),
            whole((row_count, 1), jnp.int32),
            whole((row_count, 1), F32),
        ],
        1000 * row_count,
        lengths,
        t_index,
        specs=[pl.BlockSpec(memory_space=pltpu.SMEM)] * 2,
    )

    rows, scale, triples, pairs = project(blocks, None, start_time)
    terms = attend(triples, pairs)
    student_terms = call(
        functools.partial(terms_kernel, n_tp),
        [whole((row_count, width))] * n_tp,
        2 * row_count * width * inner,
        rows, student_weight, scale,
    )
    held_s = halve(student_terms)
    held = halve(terms)
    other = {k ^ top_bit: tp_swap(held[k], top_bit) for k in sorted(held, reverse=True)}
    velocity = tuple([low[k] for k in range(n_tp)] for low in map(spread_low, (held, other)))
    _, _, triples, pairs = project(blocks, velocity, start_time)
    other_s = tp_swap(held_s[top_bit], top_bit)
    terms = attend(triples, pairs)
    (student,) = call(
        functools.partial(add_kernel, 1),
        [whole((row_count, width))],
        1000 * row_count,
        held_s[0], other_s,
    )
    held1 = halve(terms)
    other1 = tp_swap(held1[top_bit], top_bit)
    target, part = call(
        loss_kernel,
        [whole((row_count, width)), whole((8, 128), F32)],
        10 * row_count * width,
        held[0], other[0], held1[0], other1, student, own_rows,
    )
    part = part + tp_swap(part, 1)
    for bit in bits_of(n_tp)[1:-1]:
        part = part + tp_swap(part, bit)

    def both(value, seq_mask, tp_mask):
        return lax.ppermute(
            value,
            ("seq", "tp"),
            [
                (s * n_tp + t, (s ^ seq_mask) * n_tp + (t ^ tp_mask))
                for s in range(n_seq)
                for t in range(n_tp)
            ],
        )

    part = (part + both(part, 0, top_bit)) + (both(part, 1, 0) + both(part, 1, top_bit))
    low = n_seq // 4
    part = (part + seq_swap(part, low)) + (seq_swap(part, 2 * low) + seq_swap(part, 3 * low))
    image_sum = part[0, : lengths.shape[0]]
    loss = jnp.mean(image_sum / (lengths.astype(F32) * inner))
    return (target, student, loss)


def solution(mesh):
    placed = (
        P("seq", "tp"),
        P(),
        P(),
        P(),
        P(None, "tp"),
        P(None, "tp"),
        P(None, "tp"),
        P("tp", None),
        P(),
        P(),
        P("tp", None),
    )

    def body(*arguments):
        latents, q_weight, q_gain = arguments[0], arguments[4], arguments[8]
        n_seq, n_tp = mesh.shape["seq"], mesh.shape["tp"]
        heads_here = q_weight.shape[1] // q_gain.shape[0]
        fused = (
            latents.shape[1] % 128 == 0
            and q_gain.shape[0] == 128
            and n_seq == 2 * heads_here == 8
            and n_tp in (2, 4)
        )
        run = on_device_fused if fused else on_device
        return run(dict(mesh.shape), *arguments)

    return jax.shard_map(
        body,
        mesh=mesh,
        in_specs=placed,
        out_specs=(P("seq", "tp"), P("seq", "tp"), P()),
        check_vma=False,
    )
```

```python
import functools
import math

import jax
import jax.numpy as jnp
from jax import lax
from jax.experimental import pallas as pl
from jax.experimental.pallas import tpu as pltpu
from jax.sharding import PartitionSpec as P


TGRID = 8
epsilon = 1e-06
kinetic_weight = 0.1
F32, BF16 = jnp.float32, jnp.bfloat16
AHEAD, BEHIND = (2, 0), (3, 1)
KERNEL_VMEM = 16 * 1024 * 1024


def image_index(positions, image_ends):
    return jnp.sum((positions[:, None] >= image_ends[None, :]).astype(jnp.int32), axis=1)


def swap(value, axis, size, mask):
    return lax.ppermute(value, axis, [(i, i ^ mask) for i in range(size)])


def bits_of(size):
    return [1 << b for b in range(size.bit_length() - 1)]


def gather_blocks(own, axis, size):
    blocks = {0: own}
    for bit in reversed(bits_of(size)):
        for k in list(blocks):
            blocks[k ^ bit] = swap(blocks[k], axis, size, bit)
    return [blocks[k] for k in range(size)]


def in_order(blocks, index):
    size = len(blocks)
    current = list(blocks)
    for bit in bits_of(size):
        flip = (index & bit) != 0
        current = [jnp.where(flip, current[k ^ bit], current[k]) for k in range(size)]
    return current


def reduce_blocks(terms, axis, size, keep_last):
    held = dict(enumerate(terms))
    bits = bits_of(size)
    for bit in bits:
        last = keep_last and bit == bits[-1]
        sent = {k: swap(held[k].astype(BF16), axis, size, bit) for k in held if last or k & bit}
        if last:
            held = {k: held[k].astype(BF16).astype(F32) + sent[k ^ bit].astype(F32) for k in held}
        else:
            held = {
                k: held[k].astype(BF16).astype(F32) + sent[k ^ bit].astype(F32)
                for k in held
                if not k & bit
            }
    return held


def head_norm(projected, gain):
    shaped = projected.reshape(projected.shape[0], -1, gain.shape[0])
    normed = shaped * lax.rsqrt(jnp.mean(shaped * shaped, axis=-1, keepdims=True) + epsilon) * gain
    return normed.astype(BF16)


def on_device(
    mesh_shape,
    latents,
    lengths,
    t_index,
    mod_scale,
    q_weight,
    k_weight,
    v_weight,
    out_weight,
    q_gain,
    k_gain,
    student_weight,
):
    n_seq, n_tp = mesh_shape["seq"], mesh_shape["tp"]
    row_count, width_here = latents.shape
    head_dim = q_gain.shape[0]
    heads_here = q_weight.shape[1] // head_dim
    tp_index = lax.axis_index("tp")
    seq_index = lax.axis_index("seq")
    image_ends = jnp.cumsum(lengths)
    score_scale = 1.0 / math.sqrt(head_dim)
    step_size = 1.0 / TGRID

    spread = math.gcd(heads_here, n_seq)
    groups = n_seq // spread
    heads_kept = heads_here // spread
    twisted = groups == 2 and spread >= 4
    group_index = seq_index // spread
    head_block = seq_index % spread
    if twisted:
        head_block = head_block ^ (group_index * 2)

    def rows_image(source):
        return image_index(source * row_count + jnp.arange(row_count, dtype=jnp.int32), image_ends)

    query_image = rows_image(seq_index)
    one_hot = (
        query_image[:, None] == jnp.arange(lengths.shape[0], dtype=jnp.int32)[None, :]
    ).astype(F32)
    start_times = jnp.sum(one_hot * (t_index.astype(F32) / TGRID)[None, :], axis=1)

    group_image = jnp.concatenate([rows_image(seq_index ^ m) for m in range(spread)])
    if groups == 2:
        partner_mask = spread ^ 2 if twisted else spread
        key_image = jnp.concatenate(
            [group_image] + [rows_image(seq_index ^ partner_mask ^ m) for m in range(spread)]
        )
    else:
        key_image = jnp.concatenate(
            [
                rows_image((seq_index % spread ^ m) + g * spread)
                for g in range(groups)
                for m in range(spread)
            ]
        )
    same_image = group_image[:, None] == key_image[None, :]

    def attention(queries, key_rows, value_rows):
        wide = heads_kept * head_dim
        packed = jnp.concatenate(
            [
                part.reshape(row_count, spread, 1, wide)
                for part in (queries, key_rows, value_rows)
            ],
            axis=2,
        )
        received = []
        for m in range(spread):
            piece = lax.dynamic_index_in_dim(packed, head_block ^ m, 1, keepdims=False)
            piece = piece.reshape(row_count, 3 * wide)
            received.append(piece if m == 0 else swap(piece, "seq", n_seq, m))
        own = jnp.concatenate(received, axis=0)
        group_q, group_kv = own[:, :wide], own[:, wide:]
        if groups == 2:
            other = swap(group_kv, "seq", n_seq, partner_mask)
            whole_kv = jnp.concatenate([group_kv, other], axis=0)
        elif groups == 1:
            whole_kv = group_kv
        else:
            whole_kv = lax.all_gather(
                group_kv,
                "seq",
                axis=0,
                tiled=True,
                axis_index_groups=[
                    [a + g * spread for g in range(groups)] for a in range(spread)
                ],
            )
        outs = []
        for h in range(heads_kept):
            cut = slice(h * head_dim, (h + 1) * head_dim)
            q_h, k_h = group_q[:, cut], whole_kv[:, :wide][:, cut]
            v_h = whole_kv[:, wide:][:, cut]
            scores = jnp.dot(q_h, k_h.T, preferred_element_type=F32) * score_scale
            scores = jnp.where(same_image, scores, -1e30)
            highest = jnp.max(scores, axis=1, keepdims=True)
            weights = jnp.where(same_image, jnp.exp(scores - highest), 0.0)
            totals = jnp.sum(weights, axis=1, keepdims=True)
            mixed = jnp.dot(weights.astype(BF16), v_h, preferred_element_type=F32)
            outs.append((mixed / totals).astype(BF16))
        result = jnp.concatenate(outs, axis=1) if len(outs) > 1 else outs[0]
        back = []
        for m in range(spread):
            piece = result[m * row_count : (m + 1) * row_count]
            back.append(piece if m == 0 else swap(piece, "seq", n_seq, m))
        return jnp.concatenate(in_order(back, head_block), axis=1)

    def terms_of(left, right):
        product = jnp.dot(left, right, preferred_element_type=F32)
        return [
            lax.dynamic_slice_in_dim(product, (tp_index ^ k) * width_here, width_here, 1)
            for k in range(n_tp)
        ]

    def teacher(state_blocks, times):
        state32 = jnp.concatenate(in_order(state_blocks, tp_index), axis=1).astype(F32)
        normed = state32 * lax.rsqrt(jnp.mean(state32 * state32, axis=1, keepdims=True) + epsilon)
        hidden = (normed * (1.0 + times[:, None] * mod_scale[None, :])).astype(BF16)
        queries = head_norm(jnp.dot(hidden, q_weight, preferred_element_type=F32), q_gain)
        key_rows = head_norm(jnp.dot(hidden, k_weight, preferred_element_type=F32), k_gain)
        value_rows = jnp.dot(hidden, v_weight, preferred_element_type=F32).astype(BF16)
        mixed = attention(queries, key_rows, value_rows)
        return terms_of(mixed, out_weight), hidden

    def step(block, velocity):
        return (block.astype(F32) + step_size * velocity.astype(F32)).astype(BF16)

    blocks = gather_blocks(latents, "tp", n_tp)
    terms, first_hidden = teacher(blocks, start_times)
    held = reduce_blocks(terms, "tp", n_tp, True)
    velocity0 = held[0].astype(BF16)
    moved = {k: step(blocks[k], held[k].astype(BF16)) for k in held}
    for bit in reversed(bits_of(n_tp)[:-1]):
        for k in list(moved):
            moved[k ^ bit] = swap(moved[k], "tp", n_tp, bit)
    terms, _ = teacher([moved[k] for k in range(n_tp)], start_times + step_size)
    velocity1 = reduce_blocks(terms, "tp", n_tp, False)[0].astype(BF16)

    columns = lax.dynamic_slice_in_dim(first_hidden, tp_index * width_here, width_here, 1)
    student = reduce_blocks(terms_of(columns, student_weight), "tp", n_tp, False)[0].astype(BF16)

    target = (0.5 * (velocity0.astype(F32) + velocity1.astype(F32))).astype(BF16)
    student32 = student.astype(F32)
    residual = student32 - target.astype(F32)
    per_token = jnp.sum(residual * residual, axis=1) + kinetic_weight * jnp.sum(
        student32 * student32, axis=1
    )
    image_sum = jnp.sum(one_hot * per_token[:, None], axis=0)
    for bit in bits_of(n_tp):
        image_sum = image_sum + swap(image_sum, "tp", n_tp, bit)
    for bit in bits_of(n_seq):
        image_sum = image_sum + swap(image_sum, "seq", n_seq, bit)
    loss = jnp.mean(image_sum / (lengths.astype(F32) * mod_scale.shape[0]))
    return (target, student, loss)


def whole(shape, dtype=BF16):
    return jax.ShapeDtypeStruct(shape, dtype)


VM = pl.BlockSpec(memory_space=pltpu.VMEM)


def call(body, outs, flops, *operands, specs=None):
    size = sum(math.prod(a.shape) * a.dtype.itemsize for a in operands)
    return pl.pallas_call(
        body,
        out_shape=outs,
        in_specs=specs or [VM] * len(operands),
        out_specs=jax.tree.map(lambda _: VM, outs),
        compiler_params=pltpu.CompilerParams(vmem_limit_bytes=KERNEL_VMEM),
        cost_estimate=pl.CostEstimate(flops=flops, bytes_accessed=size, transcendentals=0),
    )(*operands)


def head_at(block, m, width):
    return pl.ds(pl.multiple_of((block ^ m) * width, width), width)


def normed_head(raw, gain):
    return (raw * lax.rsqrt(jnp.mean(raw * raw, axis=1, keepdims=True) + epsilon) * gain).astype(
        BF16
    )


def head_block_of(spread):
    return lax.rem(lax.axis_index("seq"), spread)


def setup_kernel(plan, images, count, *refs):
    n_tp, _, spread, _, _ = plan
    length_ref, index_ref, refs = refs[0], refs[1], refs[2:]
    sources, targets, refs = refs[:count], refs[count : 2 * count], refs[2 * count :]
    near_rows, near_keys, far_keys, time_ref, weight_ref, sems = refs
    copies = [
        pltpu.make_async_copy(source, target, sems.at[i])
        for i, (source, target) in enumerate(zip(sources, targets))
    ]
    for copy in copies:
        copy.start()
    row_count, width = time_ref.shape[0], sources[0].shape[1]
    seq_index = lax.axis_index("seq")
    ends = [length_ref[0]]
    for i in range(1, images):
        ends.append(ends[-1] + length_ref[i])

    def image_of(shape, axis, source):
        places = lax.broadcasted_iota(jnp.int32, shape, axis)
        blocks = lax.div(places, row_count)
        places = ((source ^ blocks) - blocks) * row_count + places
        return sum((places >= end).astype(jnp.int32) for end in ends)

    near_rows[...] = image_of(near_rows.shape, 0, seq_index)
    near_keys[...] = image_of(near_keys.shape, 1, seq_index)
    far_keys[...] = image_of(far_keys.shape, 1, seq_index ^ spread)
    own = image_of(time_ref.shape, 0, seq_index)
    time = jnp.zeros(own.shape, F32)
    length = jnp.ones(own.shape, F32)
    for i in range(images):
        time = jnp.where(own == i, index_ref[i].astype(F32) / TGRID, time)
        length = jnp.where(own == i, length_ref[i].astype(F32), length)
    time_ref[...] = time
    weight_ref[...] = 1.0 / (length * (n_tp * width * images))
    for copy in copies:
        copy.wait()


def setup(plan, lengths, t_index, row_count, *arrays):
    spread = plan[2]
    count, grouped = len(arrays), spread * row_count
    size = sum(math.prod(a.shape) * a.dtype.itemsize for a in arrays)
    outs = [whole(a.shape, a.dtype) for a in arrays] + [
        whole((grouped, 1), jnp.int32),
        whole((1, grouped), jnp.int32),
        whole((1, grouped), jnp.int32),
        whole((row_count, 1), F32),
        whole((row_count, 1), F32),
    ]
    results = pl.pallas_call(
        functools.partial(setup_kernel, plan, lengths.shape[0], count),
        out_shape=outs,
        in_specs=[pl.BlockSpec(memory_space=pltpu.SMEM)] * 2
        + [pl.BlockSpec(memory_space=pltpu.HBM)] * count,
        out_specs=[VM] * len(outs),
        scratch_shapes=[pltpu.SemaphoreType.DMA((count,))],
        compiler_params=pltpu.CompilerParams(vmem_limit_bytes=KERNEL_VMEM),
        cost_estimate=pl.CostEstimate(flops=200 * size, bytes_accessed=size, transcendentals=0),
    )(lengths, t_index, *[pltpu.with_memory_space_constraint(a, pltpu.HBM) for a in arrays])
    return results[:count], results[count:]


def early_kernel(plan, moving, *refs):
    part_kernel(plan, moving, 0, None, refs)


def late_kernel(plan, moving, *refs):
    rows_ref, squares_ref, *sums = refs[: 2 + plan[2] + plan[2] // 2]
    part_kernel(plan, moving, plan[0] // 2, (rows_ref, squares_ref, sums), refs[2 + len(sums) :])


def part_kernel(plan, moving, first, early, refs):
    n_tp, _, spread, head_dim, step_size = plan
    half = n_tp // 2
    state, refs = refs[:half], refs[half:]
    if moving:
        near, far, refs = refs[:half], refs[half : 2 * half], refs[2 * half :]
    time_ref, mod_ref, q_ref, k_ref, v_ref, q_gain, k_gain, rows_ref, scale_ref = refs[:9]
    outs, pairs = refs[9 : 9 + spread], refs[9 + spread :]
    tp_index = lax.axis_index("tp")
    block = head_block_of(spread)
    width = state[0].shape[1]
    times = time_ref[...]
    if moving:
        times = times + step_size
    squares = early[1][...] if early else jnp.zeros_like(times)
    for k in range(half):
        x = state[k][...].astype(F32)
        if moving:
            velocity = (near[k][...].astype(F32) + far[k][...].astype(F32)).astype(BF16)
            x = (x + step_size * velocity.astype(F32)).astype(BF16).astype(F32)
        squares = squares + jnp.sum(x * x, axis=1, keepdims=True)
        mod = mod_ref[:, head_at(tp_index, first + k, width)]
        rows_ref[:, k * width : (k + 1) * width] = (x * (1.0 + times * mod)).astype(BF16)
    scale = lax.rsqrt(squares / (n_tp * width) + epsilon) if early else None
    scale_ref[...] = scale if early else squares

    def project(pieces, before):
        total = before[...] if early else None
        for k in range(half):
            rows = head_at(tp_index, first + k, width)
            weight = jnp.concatenate(
                [ref[rows, head_at(block, m, head_dim)] for ref, m in pieces], axis=1
            )
            part = jnp.dot(
                rows_ref[:, k * width : (k + 1) * width], weight, preferred_element_type=F32
            )
            total = part if total is None else total + part
        return total * scale if early else total

    sums = early[2] if early else [None] * (spread + spread // 2)
    for m in range(spread):
        total = project([(k_ref, m), (v_ref, m)], sums[m])
        if not early:
            outs[m][...] = total
            continue
        keys = normed_head(total[:, :head_dim], k_gain[...])
        values = total[:, head_dim:].astype(BF16)
        outs[m][:, head_dim : 2 * head_dim] = keys
        outs[m][:, 2 * head_dim :] = values
        pairs[m][:, :head_dim] = keys
        pairs[m][:, head_dim:] = values
    for i in range(spread // 2):
        total = project([(q_ref, 2 * i), (q_ref, 2 * i + 1)], sums[spread + i])
        if not early:
            pairs[i][...] = total
            continue
        for m in range(2):
            piece = total[:, m * head_dim : (m + 1) * head_dim]
            outs[2 * i + m][:, :head_dim] = normed_head(piece, q_gain[...])


def terms_kernel(n_tp, left_ref, right_ref, scale_ref, *outs):
    tp_index = lax.axis_index("tp")
    width = outs[0].shape[1]
    for k in range(n_tp):
        product = jnp.dot(
            left_ref[:, :width],
            right_ref[:, head_at(tp_index, k, width)],
            preferred_element_type=F32,
        )
        outs[k][...] = (product * scale_ref[...]).astype(BF16)


def add_kernel(count, *refs):
    for own, other, out in zip(refs[:count], refs[count : 2 * count], refs[2 * count :]):
        out[...] = (own[...].astype(F32) + other[...].astype(F32)).astype(BF16)


def out_kernel(plan, places, *refs):
    _, _, spread, head_dim, _ = plan
    pieces, right_ref, outs = refs[:spread], refs[spread], refs[spread + 1 :]
    tp_index = lax.axis_index("tp")
    block = head_block_of(spread)
    width = outs[0].shape[1]
    left = jnp.concatenate([piece[...] for piece in pieces], axis=1)
    for k, out in zip(places, outs):
        columns = head_at(tp_index, k, width)
        right = jnp.concatenate(
            [right_ref[head_at(block, m, head_dim), columns] for m in range(spread)], axis=0
        )
        out[...] = jnp.dot(left, right, preferred_element_type=F32).astype(BF16)


def scores_of(query, keys, query_image, key_image, head_dim):
    scores = lax.dot_general(
        query, keys, (((1,), (1,)), ((), ())), preferred_element_type=F32
    ) * (1.0 / math.sqrt(head_dim))
    return jnp.where(query_image == key_image, scores, -1e30)


def near_kernel(spread, head_dim, ahead, *refs):
    triples, pairs, refs = refs[:spread], refs[spread : spread + len(ahead)], refs[spread + len(ahead) :]
    query_image, near_image, far_image, top_ref, total_ref, sum_ref = refs
    rows = triples[0].shape[0]
    keys = jnp.concatenate(
        [triple[:, head_dim : 2 * head_dim] for triple in triples]
        + [pair[:, :head_dim] for pair in pairs],
        axis=0,
    )
    values = jnp.concatenate(
        [triple[:, 2 * head_dim :] for triple in triples] + [pair[:, head_dim:] for pair in pairs],
        axis=0,
    )
    key_image = jnp.concatenate(
        [near_image[...]] + [far_image[:, m * rows : (m + 1) * rows] for m in ahead], axis=1
    )
    for m in range(spread):
        cut = slice(m * rows, (m + 1) * rows)
        scores = scores_of(triples[m][:, :head_dim], keys, query_image[cut], key_image, head_dim)
        top = jnp.max(scores, axis=1, keepdims=True)
        weights = jnp.exp(scores - top)
        top_ref[cut] = top
        total_ref[cut] = jnp.sum(weights, axis=1, keepdims=True)
        sum_ref[cut] = jnp.dot(weights.astype(BF16), values, preferred_element_type=F32)


def far_kernel(spread, head_dim, behind, *refs):
    triples, pairs, refs = refs[:spread], refs[spread : spread + len(behind)], refs[spread + len(behind) :]
    query_image, far_image, top_ref, total_ref, sum_ref = refs[:5]
    outs = refs[5:]
    rows = triples[0].shape[0]
    keys = jnp.concatenate([pair[:, :head_dim] for pair in pairs], axis=0)
    values = jnp.concatenate([pair[:, head_dim:] for pair in pairs], axis=0)
    key_image = jnp.concatenate([far_image[:, m * rows : (m + 1) * rows] for m in behind], axis=1)
    for m in [*range(1, spread), 0]:
        cut = slice(m * rows, (m + 1) * rows)
        scores = scores_of(triples[m][:, :head_dim], keys, query_image[cut], key_image, head_dim)
        old = top_ref[cut]
        top = jnp.maximum(old, jnp.max(scores, axis=1, keepdims=True))
        weights = jnp.exp(scores - top)
        fade = jnp.exp(old - top)
        total = total_ref[cut] * fade + jnp.sum(weights, axis=1, keepdims=True)
        mixed = sum_ref[cut] * fade + jnp.dot(
            weights.astype(BF16), values, preferred_element_type=F32
        )
        outs[m][...] = (mixed / total).astype(BF16)


def base_kernel(near0, far0, near_s, far_s, student_ref, base_ref):
    width = student_ref.shape[1]
    student = (near_s[...].astype(F32) + far_s[...].astype(F32)).astype(BF16)
    student_ref[...] = student
    base_ref[:, :width] = (near0[...].astype(F32) + far0[...].astype(F32)).astype(BF16)
    base_ref[:, width:] = student


def loss_kernel(near1, far1, base_ref, weight_ref, target_ref, part_ref):
    width = target_ref.shape[1]
    velocity0 = base_ref[:, :width].astype(F32)
    velocity1 = (near1[...].astype(F32) + far1[...].astype(F32)).astype(BF16).astype(F32)
    target = (0.5 * (velocity0 + velocity1)).astype(BF16)
    target_ref[...] = target
    student = base_ref[:, width:].astype(F32)
    residual = student - target.astype(F32)
    terms = residual * residual + kinetic_weight * (student * student)
    per_token = jnp.sum(terms, axis=1, keepdims=True) * weight_ref[...]
    part_ref[...] = jnp.sum(per_token, axis=0, keepdims=True) + jnp.zeros(part_ref.shape, F32)


def on_device_fused(
    mesh_shape,
    latents,
    lengths,
    t_index,
    mod_scale,
    q_weight,
    k_weight,
    v_weight,
    out_weight,
    q_gain,
    k_gain,
    student_weight,
):
    n_seq, n_tp = mesh_shape["seq"], mesh_shape["tp"]
    row_count, width = latents.shape
    head_dim = q_gain.shape[0]
    heads_here = q_weight.shape[1] // head_dim
    inner = n_tp * width
    step_size = 1.0 / TGRID
    spread = heads_here
    plan = (n_tp, n_seq, spread, head_dim, step_size)

    grouped = spread * row_count
    mod_row = mod_scale[None, :]
    q_row, k_row = q_gain[None, :], k_gain[None, :]

    def tp_swap(value, mask):
        return swap(value, "tp", n_tp, mask)

    def seq_swap(value, mask):
        return swap(value, "seq", n_seq, mask)

    def half_call(body, state, velocity, first, before, outs, flops):
        half = slice(first, first + n_tp // 2)
        operands = list(before) + list(state[half])
        if velocity is not None:
            operands += velocity[0][half] + velocity[1][half]
        return call(
            functools.partial(body, plan, velocity is not None),
            [whole((row_count, inner // 2)), whole((row_count, 1), F32)] + outs,
            flops,
            *operands, start_time, mod_row, q_weight, k_weight, v_weight, q_row, k_row,
        )

    def project(state, velocity):
        flops = 3 * row_count * inner * spread * head_dim
        wide = whole((row_count, 2 * head_dim), F32)
        early = half_call(
            early_kernel, state, velocity, 0, (), [wide] * (spread + spread // 2), flops
        )
        late = half_call(
            late_kernel, state, velocity, n_tp // 2, early,
            [whole((row_count, 3 * head_dim))] * spread
            + [whole((row_count, 2 * head_dim))] * spread,
            flops,
        )
        return early[0], late[1], late[2 : 2 + spread], late[2 + spread :]

    def attend(triples, pairs):
        far_pairs, near_triples = [], [triples[0]]
        for m in range(spread):
            far_pairs.append(seq_swap(pairs[m], spread ^ m))
        for m in range(1, spread):
            near_triples.append(seq_swap(triples[m], m))
        flops = 4 * grouped**2 * head_dim
        sums = call(
            functools.partial(near_kernel, spread, head_dim, AHEAD),
            [whole((grouped, 1), F32)] * 2 + [whole((grouped, head_dim), F32)],
            flops,
            *near_triples, *[far_pairs[m] for m in AHEAD], near_rows, near_keys, far_keys,
        )
        pieces = call(
            functools.partial(far_kernel, spread, head_dim, BEHIND),
            [whole((row_count, head_dim))] * spread,
            flops,
            *near_triples, *[far_pairs[m] for m in BEHIND], near_rows, far_keys, *sums,
        )
        back = [pieces[0]]
        for m in range(1, spread):
            back.append(seq_swap(pieces[m], m))
        terms = [None] * n_tp
        for places in ((3, 2), (1, 0)):
            results = call(
                functools.partial(out_kernel, plan, places),
                [whole((row_count, width))] * len(places),
                len(places) * 2 * row_count * spread * head_dim * width,
                *back, out_weight,
            )
            for k, result in zip(places, results):
                terms[k] = result
        return terms

    def halve(terms):
        held = {}
        for k in (2, 0):
            other_term = tp_swap(terms[k ^ 1], 1)
            (held[k],) = call(
                functools.partial(add_kernel, 1),
                [whole((row_count, width))],
                1000 * row_count,
                terms[k], other_term,
            )
        return held

    def spread_low(held):
        held = dict(held)
        for bit in reversed(bits_of(n_tp)[:-1]):
            for k in list(held):
                held[k ^ bit] = tp_swap(held[k], bit)
        return held

    top_bit = n_tp // 2
    top_block = tp_swap(latents, top_bit)
    held = spread_low({0: latents}) | spread_low({top_bit: top_block})
    blocks = [held[k] for k in range(n_tp)]
    fetched, places = setup(
        plan, lengths, t_index, row_count,
        latents, q_weight, k_weight, v_weight, mod_row, q_row, k_row,
    )
    blocks[0], q_weight, k_weight, v_weight, mod_row, q_row, k_row = fetched
    near_rows, near_keys, far_keys, start_time, loss_weight = places
    rows, scale, triples, pairs = project(blocks, None)
    terms = attend(triples, pairs)
    student_terms = call(
        functools.partial(terms_kernel, n_tp),
        [whole((row_count, width))] * n_tp,
        2 * row_count * width * inner,
        rows, student_weight, scale,
    )
    held_s = halve(student_terms)
    held = halve(terms)
    other = {}
    for k in (2, 0):
        other[k ^ top_bit] = tp_swap(held[k], top_bit)
    velocity = tuple([low[k] for k in range(n_tp)] for low in map(spread_low, (held, other)))
    _, _, triples, pairs = project(blocks, velocity)
    other_s = tp_swap(held_s[top_bit], top_bit)
    terms = attend(triples, pairs)
    student, base = call(
        base_kernel,
        [whole((row_count, width)), whole((row_count, 2 * width))],
        10 * row_count * width,
        held[0], other[0], held_s[0], other_s,
    )
    held1 = halve(terms)
    other1 = tp_swap(held1[top_bit], top_bit)
    target, part = call(
        loss_kernel,
        [whole((row_count, width)), whole((8, 128), F32)],
        10 * row_count * width,
        held1[0], other1, base, loss_weight,
    )
    part = part + tp_swap(part, 1)

    def both(value, seq_mask, tp_mask):
        return lax.ppermute(
            value,
            ("seq", "tp"),
            [
                (s * n_tp + t, (s ^ seq_mask) * n_tp + (t ^ tp_mask))
                for s in range(n_seq)
                for t in range(n_tp)
            ],
        )

    part = (part + both(part, 0, top_bit)) + (both(part, 1, 0) + both(part, 1, top_bit))
    low = n_seq // 4
    part = (part + seq_swap(part, low)) + (seq_swap(part, 2 * low) + seq_swap(part, 3 * low))
    loss = part[0, 0]
    return (target, student, loss)


def solution(mesh):
    placed = (
        P("seq", "tp"),
        P(),
        P(),
        P(),
        P(None, "tp"),
        P(None, "tp"),
        P(None, "tp"),
        P("tp", None),
        P(),
        P(),
        P("tp", None),
    )

    def body(*arguments):
        latents, q_weight, q_gain = arguments[0], arguments[4], arguments[8]
        n_seq, n_tp = mesh.shape["seq"], mesh.shape["tp"]
        heads_here = q_weight.shape[1] // q_gain.shape[0]
        fused = (
            latents.shape[1] % 128 == 0
            and q_gain.shape[0] == 128
            and n_seq == 2 * heads_here == 8
            and n_tp == 4
        )
        run = on_device_fused if fused else on_device
        return run(dict(mesh.shape), *arguments)

    return jax.shard_map(
        body,
        mesh=mesh,
        in_specs=placed,
        out_specs=(P("seq", "tp"), P("seq", "tp"), P()),
        check_vma=False,
    )
```
